128 devices in a mesh: rep: 1, tp: 2 (over core), dp: 64 (over z, y, x).
Axes of the slice: x: 4, y: 4, z: 4, core: 2. Of those that a mesh axis runs over, the one named last changes fastest.
Arguments:
- x: bfloat16 [128, 2560], P(('rep', 'dp'))
- lengths: int32 [128], P(('rep', 'dp'))
- cache0: bfloat16 [128, 4096, 288], P(('rep', 'dp'))
- cache1: bfloat16 [128, 4096, 288], P(('rep', 'dp'))
- attn_gain: float32 [2, 2560], replicated
- kv_gain: float32 [2, 256], replicated
- q_gain: float32 [2, 768], replicated
- ffn_gain: float32 [2, 2560], replicated
- w_dkv: bfloat16 [2, 2560, 288], replicated
- w_qa: bfloat16 [2, 2560, 768], replicated
- w_qb: bfloat16 [2, 768, 3840], P(None, None, 'tp')
- w_uk: bfloat16 [2, 40, 64, 256], P(None, 'tp')
- w_uv: bfloat16 [2, 40, 256, 64], P(None, 'tp')
- w_o: bfloat16 [2, 2560, 2560], P(None, 'tp')
- w_gate: bfloat16 [2, 2560, 6400], replicated
- w_up: bfloat16 [2, 2560, 6400], replicated
- w_down: bfloat16 [2, 6400, 2560], replicated
Outputs:
- output 1: bfloat16 [128, 2560], P(('rep', 'dp'))
- output 2: bfloat16 [128, 4096, 288], P(('rep', 'dp'))
- output 3: bfloat16 [128, 4096, 288], P(('rep', 'dp'))
All inputs are finite; a program needn't handle non-finite values.
Results may differ from the reference program's by a relative error of at most 0.0143243.
Values are sent between devices in bfloat16 or wider.
A program may use at most 1 GiB of HBM per device.

```python
import jax
import jax.numpy as jnp
from jax import lax

MODEL_DIM = 2560
FFN_DIM = 6400
NUM_HEADS = 40
Q_LORA = 768
KV_LORA = 256
ROPE_DIM = 32
NOPE_DIM = 64
V_DIM = 64
BATCH = 128
SEQ_LEN = 4096
LAYER_COUNT = 2

LAT_WIDTH = KV_LORA + ROPE_DIM
QK_WIDTH = NOPE_DIM + ROPE_DIM
NORM_EPS = 1e-6
ROPE_BASE = 10000.0


def rms_norm(values, gain_vec):
    wide_vals = values.astype(jnp.float32)
    inv_rms = lax.rsqrt(jnp.mean(wide_vals * wide_vals, axis=-1, keepdims=True) + NORM_EPS)
    return (wide_vals * inv_rms * gain_vec.astype(jnp.float32)).astype(jnp.bfloat16)


def rope_tables(lengths):
    half_dim = ROPE_DIM // 2
    inv_freq = ROPE_BASE ** (-2.0 * jnp.arange(half_dim).astype(jnp.float32) / ROPE_DIM)
    angles = lengths.astype(jnp.float32)[:, None] * inv_freq[None, :]
    return jnp.cos(angles), jnp.sin(angles)


def rotate(values, cos_tab, sin_tab):
    half_dim = values.shape[-1] // 2
    first_half = values[..., :half_dim]
    second_half = values[..., half_dim:]
    return jnp.concatenate([first_half * cos_tab - second_half * sin_tab, second_half * cos_tab + first_half * sin_tab], axis=-1)


def row_attention(row_query, row_cache, row_len):
    scores = jnp.einsum('hk,tk->ht', row_query.astype(jnp.float32), row_cache.astype(jnp.float32)) * QK_WIDTH ** -0.5
    valid_mask = jnp.arange(SEQ_LEN)[None, :] <= row_len
    att_probs = jax.nn.softmax(jnp.where(valid_mask, scores, -1e30), axis=-1).astype(jnp.bfloat16)
    return jnp.einsum('ht,tk->hk', att_probs.astype(jnp.float32), row_cache[:, :KV_LORA].astype(jnp.float32)).astype(jnp.bfloat16)


def layer_step(x_rows, lengths, cache, cos_tab, sin_tab, attn_g, kv_g, q_g, ffn_g, w_dkv, w_qa, w_qb, w_uk, w_uv, w_o, w_gate, w_up, w_down):
    normed = rms_norm(x_rows, attn_g)
    kv_lat = jnp.dot(normed, w_dkv, preferred_element_type=jnp.float32)
    new_entry = jnp.concatenate([rms_norm(kv_lat[:, :KV_LORA], kv_g), rotate(kv_lat[:, KV_LORA:], cos_tab, sin_tab).astype(jnp.bfloat16)], axis=-1)
    is_slot = (jnp.arange(SEQ_LEN)[None, :] == lengths[:, None])[:, :, None]
    new_cache = jnp.where(is_slot, new_entry[:, None, :], cache)
    q_low = rms_norm(jnp.dot(normed, w_qa, preferred_element_type=jnp.float32), q_g)
    q_full = jnp.dot(q_low, w_qb, preferred_element_type=jnp.float32).reshape(BATCH, NUM_HEADS, QK_WIDTH)
    q_nope = q_full[:, :, :NOPE_DIM].astype(jnp.bfloat16)
    q_rot = rotate(q_full[:, :, NOPE_DIM:], cos_tab[:, None, :], sin_tab[:, None, :]).astype(jnp.bfloat16)
    q_lat = jnp.einsum('bhn,hnk->bhk', q_nope.astype(jnp.float32), w_uk.astype(jnp.float32)).astype(jnp.bfloat16)
    query_vec = jnp.concatenate([q_lat, q_rot], axis=-1)
    lat_out = lax.map(lambda row_item: row_attention(row_item[0], row_item[1], row_item[2]), (query_vec, new_cache, lengths))
    head_out = jnp.einsum('bhk,hkv->bhv', lat_out.astype(jnp.float32), w_uv.astype(jnp.float32)).astype(jnp.bfloat16)
    attn_out = jnp.dot(head_out.reshape(BATCH, NUM_HEADS * V_DIM), w_o, preferred_element_type=jnp.float32)
    x_mid = (x_rows.astype(jnp.float32) + attn_out).astype(jnp.bfloat16)
    ffn_in = rms_norm(x_mid, ffn_g)
    hidden = (jax.nn.silu(jnp.dot(ffn_in, w_gate, preferred_element_type=jnp.float32)) * jnp.dot(ffn_in, w_up, preferred_element_type=jnp.float32)).astype(jnp.bfloat16)
    ffn_out = jnp.dot(hidden, w_down, preferred_element_type=jnp.float32)
    return (x_mid.astype(jnp.float32) + ffn_out).astype(jnp.bfloat16), new_cache


def draw_lengths(base_key):
    key_long, key_short, key_pick = jax.random.split(base_key, 3)
    long_len = jax.random.randint(key_long, (BATCH,), 0, SEQ_LEN)
    short_len = jax.random.randint(key_short, (BATCH,), 0, min(4, SEQ_LEN))
    pick_short = jax.random.randint(key_pick, (BATCH,), 0, 2)
    row_ids = jnp.arange(BATCH)
    drawn = jnp.where(pick_short == 1, short_len, long_len)
    drawn = jnp.where(row_ids == 0, SEQ_LEN - 1, drawn)
    drawn = jnp.where(row_ids == 1, 0, drawn)
    return drawn.astype(jnp.int32)


def draw_cache(base_key, lengths):
    key_common, key_noise = jax.random.split(base_key)
    common = jax.random.normal(key_common, (BATCH, 1, LAT_WIDTH), jnp.float32)
    slot_noise = jax.random.normal(key_noise, (BATCH, SEQ_LEN, LAT_WIDTH), jnp.float32)
    filled = (jnp.arange(SEQ_LEN)[None, :] < lengths[:, None])[:, :, None]
    return jnp.where(filled, 0.8 * common + 0.6 * slot_noise, 40.0 * slot_noise).astype(jnp.bfloat16)


def normal_weight(base_key, shape, fan_in):
    return (jax.random.normal(base_key, shape, jnp.float32) * fan_in ** -0.5).astype(jnp.bfloat16)


def setup_inputs(seed: int = 0, part: int = 0) -> dict:
    shared = jax.random.split(jax.random.key(seed), 13)
    part_keys = jax.random.split(jax.random.fold_in(jax.random.key(seed + 1), part), 4)
    lengths = draw_lengths(part_keys[1])
    return {
        'x': jax.random.normal(part_keys[0], (BATCH, MODEL_DIM), jnp.float32).astype(jnp.bfloat16),
        'lengths': lengths,
        'cache0': draw_cache(part_keys[2], lengths),
        'cache1': draw_cache(part_keys[3], lengths),
        'attn_gain': jax.random.uniform(shared[0], (LAYER_COUNT, MODEL_DIM), jnp.float32, 0.4, 1.6),
        'kv_gain': jax.random.uniform(shared[1], (LAYER_COUNT, KV_LORA), jnp.float32, 0.4, 1.6),
        'q_gain': jax.random.uniform(shared[2], (LAYER_COUNT, Q_LORA), jnp.float32, 0.4, 1.6),
        'ffn_gain': jax.random.uniform(shared[3], (LAYER_COUNT, MODEL_DIM), jnp.float32, 0.4, 1.6),
        'w_dkv': normal_weight(shared[4], (LAYER_COUNT, MODEL_DIM, LAT_WIDTH), MODEL_DIM),
        'w_qa': normal_weight(shared[5], (LAYER_COUNT, MODEL_DIM, Q_LORA), MODEL_DIM),
        'w_qb': normal_weight(shared[6], (LAYER_COUNT, Q_LORA, NUM_HEADS * QK_WIDTH), Q_LORA),
        'w_uk': normal_weight(shared[7], (LAYER_COUNT, NUM_HEADS, NOPE_DIM, KV_LORA), NOPE_DIM),
        'w_uv': normal_weight(shared[8], (LAYER_COUNT, NUM_HEADS, KV_LORA, V_DIM), KV_LORA),
        'w_o': normal_weight(shared[9], (LAYER_COUNT, NUM_HEADS * V_DIM, MODEL_DIM), NUM_HEADS * V_DIM),
        'w_gate': normal_weight(shared[10], (LAYER_COUNT, MODEL_DIM, FFN_DIM), MODEL_DIM),
        'w_up': normal_weight(shared[11], (LAYER_COUNT, MODEL_DIM, FFN_DIM), MODEL_DIM),
        'w_down': normal_weight(shared[12], (LAYER_COUNT, FFN_DIM, MODEL_DIM), FFN_DIM // 2),
    }


def reference(x, lengths, cache0, cache1, attn_gain, kv_gain, q_gain, ffn_gain, w_dkv, w_qa, w_qb, w_uk, w_uv, w_o, w_gate, w_up, w_down):
    cos_tab, sin_tab = rope_tables(lengths)
    caches = [cache0, cache1]
    new_caches = []
    x_rows = x
    for layer_idx in range(LAYER_COUNT):
        x_rows, new_cache = layer_step(x_rows, lengths, caches[layer_idx], cos_tab, sin_tab, attn_gain[layer_idx], kv_gain[layer_idx], q_gain[layer_idx], ffn_gain[layer_idx], w_dkv[layer_idx], w_qa[layer_idx], w_qb[layer_idx], w_uk[layer_idx], w_uv[layer_idx], w_o[layer_idx], w_gate[layer_idx], w_up[layer_idx], w_down[layer_idx])
        new_caches.append(new_cache)
    return (x_rows, new_caches[0], new_caches[1])
```

```python
import functools

import jax
import jax.numpy as jnp
import numpy as np
from jax import lax
from jax.experimental import pallas as pl
from jax.experimental.pallas import tpu as pltpu
from jax.sharding import PartitionSpec as P

MESH = pl.DeviceIdType.MESH
NORM_EPS = 1e-6
ROPE_BASE = 10000.0
HEAD_PAD = 24
LANES = 128
VMEM_SPEC = pl.BlockSpec(memory_space=pltpu.VMEM)
SMEM_SPEC = pl.BlockSpec(memory_space=pltpu.SMEM)
ANY_SPEC = pl.BlockSpec(memory_space=pltpu.HBM)
NT = (((1,), (1,)), ((), ()))


def dot(a, b):
    return jnp.dot(a, b, preferred_element_type=jnp.float32)


def dot_nt(a, b):
    return lax.dot_general(a, b, NT, preferred_element_type=jnp.float32)


def rms(values, gain):
    inv = lax.rsqrt(jnp.mean(values * values, axis=-1, keepdims=True) + NORM_EPS)
    return (values * inv * gain).astype(jnp.bfloat16)


def rope_freq(head_width, nope, rope, width):
    half = rope // 2
    inv = ROPE_BASE ** (-2.0 * np.arange(half) / rope)
    freq = np.zeros(width + LANES)
    sign = np.zeros(width + LANES)
    starts = [h * head_width + nope for h in range(width // head_width)] + [width]
    for s in starts:
        freq[s:s + half] = inv
        freq[s + half:s + rope] = inv
        sign[s:s + half] = -1.0
        sign[s + half:s + rope] = 1.0
    return freq.astype(np.float32), sign.astype(np.float32)


def rotate_lanes(values, cos, sin, half):
    width = values.shape[-1]
    up = pltpu.roll(values, width - half, 1)
    down = pltpu.roll(values, half, 1)
    lane = lax.broadcasted_iota(jnp.int32, values.shape, 1)
    return values, up, down, lane


def attn_kernel(layer, dims, len_ref, x_ref, tab_ref, attn_g, kv_g, q_g, cache, w_dkv, w_qa, w_qb, w_uk, w_uv, w_o, part_ref, cache_out,
                dkv_b, qa_b, qb_b, uk_b, uv_b, o_b, c_b, s_b, p_b, sems, out_sems):
    rows, heads, nope, rope, lat, slots = dims
    half = rope // 2
    width = heads * (nope + rope)
    hw = nope + rope
    entry_w = lat + rope

    copies = {}

    def begin(name, src, dst, i):
        copies[name] = pltpu.make_async_copy(src, dst, sems.at[i])
        copies[name].start()

    qa_rows = w_qa.shape[1] // 2
    qb_rows = w_qb.shape[1] // 2
    o_rows = w_o.shape[1] // 4
    begin("dkv", w_dkv.at[layer], dkv_b, 0)
    for i in range(2):
        begin(f"qa{i}", w_qa.at[layer, pl.ds(i * qa_rows, qa_rows)], qa_b.at[pl.ds(i * qa_rows, qa_rows)], 1 + i)
    for i in range(2):
        begin(f"qb{i}", w_qb.at[layer, pl.ds(i * qb_rows, qb_rows)], qb_b.at[pl.ds(i * qb_rows, qb_rows)], 3 + i)
    begin("uk", w_uk.at[layer], uk_b.at[:, pl.ds(0, nope), pl.ds(0, lat)], 5)
    for r in range(rows):
        begin(f"c{r}", cache.at[r], c_b.at[r], 6 + r)
    begin("uv", w_uv.at[layer], uv_b, 8)
    for i in range(4):
        begin(f"o{i}", w_o.at[layer, pl.ds(i * o_rows, o_rows)], o_b.at[pl.ds(i * o_rows, o_rows)], 9 + i)

    uk_b[:, nope:, :lat] = jnp.zeros((heads, rope, lat), jnp.bfloat16)
    sub = lax.broadcasted_iota(jnp.int32, (heads, hw, LANES), 1)
    lan = lax.broadcasted_iota(jnp.int32, (heads, hw, LANES), 2)
    uk_b[:, :, lat:] = jnp.where(sub == lan + nope, 1.0, 0.0).astype(jnp.bfloat16)

    h = rms(x_ref[...].astype(jnp.float32), attn_g[layer:layer + 1, :])
    cos, sin = tab_ref[0], tab_ref[1]

    copies["dkv"].wait()
    kv = dot_nt(h, dkv_b[...])
    k_lat = rms(kv[:, :lat], kv_g[layer:layer + 1, :])
    k_raw = jnp.concatenate([kv[:, lat:], jnp.zeros((rows, LANES - rope), jnp.float32)], axis=1)
    lane = lax.broadcasted_iota(jnp.int32, k_raw.shape, 1)
    k_other = jnp.where(lane < half, pltpu.roll(k_raw, LANES - half, 1), pltpu.roll(k_raw, half, 1))
    k_rot = (k_raw * cos[:, width:] + k_other * sin[:, width:]).astype(jnp.bfloat16)
    entry = jnp.concatenate([k_lat.astype(jnp.float32), k_rot.astype(jnp.float32)], axis=1)
    entry = jnp.concatenate([entry, jnp.zeros((8 - rows, lat + LANES), jnp.float32)], axis=0)
    entry_t = entry.T[:entry_w]

    qa = jnp.zeros((rows, w_qa.shape[2]), jnp.float32)
    for i in range(2):
        copies[f"qa{i}"].wait()
        qa += dot(h[:, i * qa_rows:(i + 1) * qa_rows], qa_b[pl.ds(i * qa_rows, qa_rows)])
    q_low = rms(qa, q_g[layer:layer + 1, :])
    q = jnp.zeros((rows, width), jnp.float32)
    for i in range(2):
        copies[f"qb{i}"].wait()
        q += dot(q_low[:, i * qb_rows:(i + 1) * qb_rows], qb_b[pl.ds(i * qb_rows, qb_rows)])
    sin_q = sin[:, :width]
    q_other = jnp.where(sin_q < 0, 1.0, 0.0)
    lane = lax.broadcasted_iota(jnp.int32, q.shape, 1) % hw
    q_other = jnp.where(lane < nope + half, pltpu.roll(q, width - half, 1), pltpu.roll(q, half, 1))
    q = jnp.where(lane < nope, q, q * cos[:, :width] + q_other * sin_q)

    spread_shape = (HEAD_PAD, width)
    own = lax.broadcasted_iota(jnp.int32, spread_shape, 0) == lax.broadcasted_iota(jnp.int32, spread_shape, 1) // hw
    spread = jnp.concatenate([jnp.where(own, jnp.broadcast_to(q[r:r + 1], spread_shape), 0.0) for r in range(rows)], axis=0).astype(jnp.bfloat16)
    copies["uk"].wait()
    query = dot(spread, uk_b[...].reshape(width, lat + LANES))

    chunk = 1024
    pieces = slots // chunk
    scale = hw ** -0.5
    o_lat = []
    for r in range(rows):
        copies[f"c{r}"].wait()
        length = len_ref[r]
        base = pl.multiple_of(length // LANES * LANES, LANES)
        tile = c_b[r, :, pl.ds(base, LANES)].astype(jnp.float32)
        lane = lax.broadcasted_iota(jnp.int32, tile.shape, 1)
        tile = jnp.where(lane == length - base, jnp.broadcast_to(entry_t[:, r:r + 1], tile.shape), tile)
        c_b[r, :, pl.ds(base, LANES)] = tile.astype(jnp.bfloat16)

        q_r = query[r * HEAD_PAD:(r + 1) * HEAD_PAD].astype(jnp.bfloat16)
        top = jnp.full((HEAD_PAD, 1), -1e30, jnp.float32)
        for c in range(pieces):
            cols = pl.ds(c * chunk, chunk)
            s = dot(q_r[:, :lat], c_b[r, pl.ds(0, lat), cols]) + dot(q_r[:, lat:entry_w], c_b[r, pl.ds(lat, rope), cols])
            slot = lax.broadcasted_iota(jnp.int32, s.shape, 1) + c * chunk
            s = jnp.where(slot <= length, s * scale, -1e30)
            s_b[r, :, cols] = s
            top = jnp.maximum(top, jnp.max(s, axis=1, keepdims=True))
        copies[f"out{r}"] = pltpu.make_async_copy(c_b.at[r], cache_out.at[r], out_sems.at[r])
        copies[f"out{r}"].start()
        total = jnp.zeros((HEAD_PAD, 1), jnp.float32)
        for c in range(pieces):
            cols = pl.ds(c * chunk, chunk)
            e = jnp.exp(s_b[r, :, cols] - top)
            s_b[r, :, cols] = e
            total += jnp.sum(e, axis=1, keepdims=True)
        inv = 1.0 / total
        acc = jnp.zeros((HEAD_PAD, lat), jnp.float32)
        for c in range(pieces):
            cols = pl.ds(c * chunk, chunk)
            p = (s_b[r, :, cols] * inv).astype(jnp.bfloat16)
            acc += dot_nt(p, c_b[r, pl.ds(0, lat), cols])
        o_lat.append(acc)

    o_lat = jnp.concatenate(o_lat, axis=0).astype(jnp.bfloat16)
    copies["uv"].wait()
    v_dim = w_uv.shape[2]
    wide = dot_nt(o_lat, uv_b[...].reshape(heads * v_dim, lat))
    pick_shape = (HEAD_PAD, heads * v_dim)
    own = lax.broadcasted_iota(jnp.int32, pick_shape, 0) == lax.broadcasted_iota(jnp.int32, pick_shape, 1) // v_dim
    o = [jnp.sum(jnp.where(own, wide[r * HEAD_PAD:(r + 1) * HEAD_PAD], 0.0), axis=0, keepdims=True) for r in range(rows)]
    o = jnp.concatenate(o, axis=0).astype(jnp.bfloat16)
    part = jnp.zeros(part_ref.shape, jnp.float32)
    for i in range(4):
        copies[f"o{i}"].wait()
        part += dot(o[:, i * o_rows:(i + 1) * o_rows], o_b[pl.ds(i * o_rows, o_rows)])
    part_ref[...] = part
    for r in range(rows):
        copies[f"out{r}"].wait()


def attention(layer, lengths, x, tables, attn_gain, kv_gain, q_gain, cache_t, w_dkv_t, w_qa, w_qb, w_uk, w_uv_t, w_o):
    rows, model = x.shape
    heads, nope, lat = w_uk.shape[1:]
    slots = cache_t.shape[2]
    rope = cache_t.shape[1] - lat
    bf = jnp.bfloat16
    width = w_qb.shape[2]
    dims = (rows, heads, nope, rope, lat, slots)
    return pl.pallas_call(
        functools.partial(attn_kernel, layer, dims),
        name=f"attn{layer}",
        out_shape=(jax.ShapeDtypeStruct((rows, model), jnp.float32), jax.ShapeDtypeStruct(cache_t.shape, bf)),
        in_specs=[SMEM_SPEC] + [VMEM_SPEC] * 5 + [ANY_SPEC] * 7,
        out_specs=(VMEM_SPEC, ANY_SPEC),
        scratch_shapes=[
            pltpu.VMEM(w_dkv_t.shape[1:], bf),
            pltpu.VMEM(w_qa.shape[1:], bf),
            pltpu.VMEM(w_qb.shape[1:], bf),
            pltpu.VMEM((heads, nope + rope, lat + LANES), bf),
            pltpu.VMEM(w_uv_t.shape[1:], bf),
            pltpu.VMEM(w_o.shape[1:], bf),
            pltpu.VMEM(cache_t.shape, bf),
            pltpu.VMEM((rows, HEAD_PAD, slots), jnp.float32),
            pltpu.VMEM((8, LANES), bf),
            pltpu.SemaphoreType.DMA((13,)),
            pltpu.SemaphoreType.DMA((2,)),
        ],
        compiler_params=pltpu.CompilerParams(vmem_limit_bytes=62 * 2 ** 20),
        cost_estimate=pl.CostEstimate(flops=2 * 10 ** 8, bytes_accessed=26 * 10 ** 6, transcendentals=2 * 10 ** 5),
    )(lengths, x, tables, attn_gain, kv_gain, q_gain, cache_t, w_dkv_t, w_qa, w_qb, w_uk, w_uv_t, w_o)


def ffn_kernel(layer, dims, part_ref, x_ref, ffn_g, w_gate, w_up, w_down, out_ref,
               gate_b, up_b, down_b, mine_b, part_b, mid_b, send_b, sum_b, w_sems, s1, r1, s2, r2):
    ranks, tp, rows, tiles_all, tiles = dims
    members = ranks * tp
    c = lax.axis_index("tp")
    d = lax.axis_index("dp")
    pos = lax.rem(d, ranks)
    base = d - pos
    me = pos * tp + c
    start = tiles_all * me // members
    count = tiles_all * (me + 1) // members - start
    first = pl.multiple_of(jnp.minimum(start, tiles_all - tiles) * LANES, LANES)
    skip = start - jnp.minimum(start, tiles_all - tiles)

    loads = [
        pltpu.make_async_copy(w_gate.at[layer, :, pl.ds(first, tiles * LANES)], gate_b, w_sems.at[0]),
        pltpu.make_async_copy(w_up.at[layer, :, pl.ds(first, tiles * LANES)], up_b, w_sems.at[1]),
        pltpu.make_async_copy(w_down.at[layer, pl.ds(first, tiles * LANES)], down_b, w_sems.at[2]),
    ]
    for load in loads:
        load.start()

    def peer(k):
        other = lax.rem(me + k, members)
        return other // tp, lax.rem(other, tp)

    barrier = pltpu.get_barrier_semaphore()
    for k in range(1, members):
        q, t = peer(k)
        pl.semaphore_signal(barrier, inc=1, device_id={"tp": t, "dp": base + q}, device_id_type=MESH)

    keep = jnp.where(c == 0, 1.0, 0.0)
    mine = part_ref[...] + x_ref[...].astype(jnp.float32) * keep
    mine_b[...] = mine
    part_b[me] = mine
    pl.semaphore_wait(barrier, members - 1)

    sends = []
    for k in range(1, members):
        q, t = peer(k)
        sends.append(pltpu.make_async_remote_copy(
            src_ref=mine_b, dst_ref=part_b.at[me], send_sem=s1.at[k - 1], recv_sem=r1.at[k - 1],
            device_id={"tp": t, "dp": base + q}, device_id_type=MESH))
    for copy in sends:
        copy.start()
    for copy in sends:
        copy.wait_recv()

    for q in range(ranks):
        total = part_b[q * tp]
        for t in range(1, tp):
            total = total + part_b[q * tp + t]
        mid_b[q * rows:(q + 1) * rows, :] = total.astype(jnp.bfloat16).astype(jnp.float32)
    g = rms(mid_b[...], ffn_g[layer:layer + 1, :])
    loads[0].wait()
    a = dot(g, gate_b[...])
    loads[1].wait()
    b = dot(g, up_b[...])
    lane = lax.broadcasted_iota(jnp.int32, a.shape, 1)
    kept = (lane >= skip * LANES) & (lane < (skip + count) * LANES)
    u = jnp.where(kept, a * jax.nn.sigmoid(a) * b, 0.0).astype(jnp.bfloat16)
    loads[2].wait()
    partial = dot(u, down_b[...])
    for q in range(ranks):
        send_b[q] = partial[q * rows:(q + 1) * rows].astype(jnp.bfloat16)
    sum_b[me] = send_b[pos]

    returns = []
    for k in range(1, members):
        q, t = peer(k)
        returns.append(pltpu.make_async_remote_copy(
            src_ref=send_b.at[q], dst_ref=sum_b.at[me], send_sem=s2.at[k - 1], recv_sem=r2.at[k - 1],
            device_id={"tp": t, "dp": base + q}, device_id_type=MESH))
    for copy in returns:
        copy.start()
    own = part_b[pos * tp]
    for t in range(1, tp):
        own = own + part_b[pos * tp + t]
    own = own.astype(jnp.bfloat16).astype(jnp.float32)
    for copy in returns:
        copy.wait_recv()
    total = sum_b[0].astype(jnp.float32)
    for j in range(1, members):
        total = total + sum_b[j].astype(jnp.float32)
    out_ref[...] = (own + total).astype(jnp.bfloat16)
    for copy in sends + returns:
        copy.wait_send()


def ffn(layer, ranks, tp, part, x, ffn_gain, w_gate, w_up, w_down):
    rows, model = x.shape
    tiles_all = w_gate.shape[2] // LANES
    members = ranks * tp
    tiles = -(-tiles_all // members)
    width = tiles * LANES
    bf = jnp.bfloat16
    return pl.pallas_call(
        functools.partial(ffn_kernel, layer, (ranks, tp, rows, tiles_all, tiles)),
        name=f"ffn{layer}",
        out_shape=jax.ShapeDtypeStruct((rows, model), bf),
        in_specs=[VMEM_SPEC] * 3 + [ANY_SPEC] * 3,
        out_specs=VMEM_SPEC,
        scratch_shapes=[
            pltpu.VMEM((model, width), bf),
            pltpu.VMEM((model, width), bf),
            pltpu.VMEM((width, model), bf),
            pltpu.VMEM((rows, model), jnp.float32),
            pltpu.VMEM((members, rows, model), jnp.float32),
            pltpu.VMEM((ranks * rows, model), jnp.float32),
            pltpu.VMEM((ranks, rows, model), bf),
            pltpu.VMEM((members, rows, model), bf),
            pltpu.SemaphoreType.DMA((3,)),
            pltpu.SemaphoreType.DMA((members - 1,)),
            pltpu.SemaphoreType.DMA((members - 1,)),
            pltpu.SemaphoreType.DMA((members - 1,)),
            pltpu.SemaphoreType.DMA((members - 1,)),
        ],
        compiler_params=pltpu.CompilerParams(collective_id=layer, has_side_effects=True, vmem_limit_bytes=32 * 2 ** 20),
        cost_estimate=pl.CostEstimate(flops=2 * 10 ** 8, bytes_accessed=14 * 10 ** 6, transcendentals=10 ** 4),
    )(part, x, ffn_gain, w_gate, w_up, w_down)


def solution(mesh):
    tp_size = mesh.shape['tp']
    ranks = 4
    row_spec = P(('rep', 'dp'), None)
    cache_spec = P(('rep', 'dp'), None, None)
    in_specs = (row_spec, P(('rep', 'dp')), cache_spec, cache_spec, P(), P(), P(), P(), P(), P(), P(None, None, 'tp'), P(None, 'tp', None, None), P(None, 'tp', None, None), P(None, 'tp', None), P(), P(), P())
    out_specs = (row_spec, cache_spec, cache_spec)

    def local_step(x, lengths, cache0, cache1, attn_gain, kv_gain, q_gain, ffn_gain, w_dkv, w_qa, w_qb, w_uk, w_uv, w_o, w_gate, w_up, w_down):
        nope, lat = w_uk.shape[2:]
        rope = cache0.shape[2] - lat
        freq, sign = rope_freq(nope + rope, nope, rope, w_qb.shape[2])
        angles = lengths.astype(jnp.float32)[:, None] * jnp.asarray(freq)[None, :]
        tables = jnp.stack([jnp.cos(angles), jnp.sin(angles) * jnp.asarray(sign)[None, :]])
        w_dkv_t = jnp.swapaxes(w_dkv, 1, 2)
        w_uv_t = jnp.swapaxes(w_uv, 2, 3)
        new = []
        for layer, cache in enumerate((cache0, cache1)):
            part, cache_t = attention(layer, lengths, x, tables, attn_gain, kv_gain, q_gain, jnp.swapaxes(cache, 1, 2), w_dkv_t, w_qa, w_qb, w_uk, w_uv_t, w_o)
            x = ffn(layer, ranks, tp_size, part, x, ffn_gain, w_gate, w_up, w_down)
            new.append(jnp.swapaxes(cache_t, 1, 2))
        return x, new[0], new[1]

    return jax.shard_map(local_step, mesh=mesh, in_specs=in_specs, out_specs=out_specs, check_vma=False)
```

```python
import functools

import jax
import jax.numpy as jnp
import numpy as np
from jax import lax
from jax.experimental import pallas as pl
from jax.experimental.pallas import tpu as pltpu
from jax.sharding import PartitionSpec as P

MESH = pl.DeviceIdType.MESH
NORM_EPS = 1e-6
ROPE_BASE = 10000.0
HEAD_PAD = 24
LANES = 128
CHUNK = 1024
OUT_CHUNK = 512
SIDE = 4
VMEM_SPEC = pl.BlockSpec(memory_space=pltpu.VMEM)
SMEM_SPEC = pl.BlockSpec(memory_space=pltpu.SMEM)
HBM_SPEC = pl.BlockSpec(memory_space=pltpu.HBM)
NT = (((1,), (1,)), ((), ()))
F32 = jnp.float32
BF16 = jnp.bfloat16


def dot(a, b):
    return jnp.dot(a, b, preferred_element_type=F32)


def dot_nt(a, b):
    return lax.dot_general(a, b, NT, preferred_element_type=F32)


def rms(values, gain):
    inv = lax.rsqrt(jnp.mean(values * values, axis=-1, keepdims=True) + NORM_EPS)
    return (values * inv * gain).astype(BF16)


def rope_lanes(head_width, nope, rope, period):
    half = rope // 2
    turns = ROPE_BASE ** (-2.0 * np.arange(half) / rope) / (2.0 * np.pi)
    freq = np.zeros(period + LANES)
    sign = np.zeros(period + LANES)
    for s in [h * head_width + nope for h in range(period // head_width)] + [period]:
        freq[s:s + half] = turns
        freq[s + half:s + rope] = turns
        sign[s:s + half] = -1.0
        sign[s + half:s + rope] = 1.0
    mant, expo = np.frexp(freq)
    high = np.ldexp(np.floor(mant * 2.0 ** 12), expo - 12)
    table = np.zeros((8, period + LANES), np.float32)
    table[0], table[1], table[2] = high, freq - high, sign
    return table


def series(x, terms):
    out = jnp.full(x.shape, terms[-1], F32)
    for t in terms[-2::-1]:
        out = out * x + t
    return out


def cos_sin(turns):
    x = turns * np.float32(np.pi)
    x2 = x * x
    fact = np.cumprod([1.0] + list(range(1, 18)))
    s = x * series(x2, [np.float32((-1.0) ** i / fact[2 * i + 1]) for i in range(8)])
    c = series(x2, [np.float32((-1.0) ** i / fact[2 * i]) for i in range(9)])
    return 1.0 - 2.0 * s * s, 2.0 * s * c


def step_kernel(dims, len_ref, lane_ref, x_ref, attn_g, kv_g, q_g, ffn_g, cache0, cache1, w_dkv, w_qa, w_qb, w_uk, w_uv, w_o, w_gate, w_up, w_down,
                x_out, entry_out, c_out0, c_out1,
                dkv_b, qa_b, qb_b, uk_b, uv_b, o_b, gate_b, up_b, down_b, s_b, mine_b, part_b, mid_b, all_b, send_b, sum_b,
                a_sems, f_sems, ps, pr, ms, mr, rs, rr):
    layers, rows, heads, nope, rope, lat, slots, tiles_all, tiles, ranks, tp, period = dims
    half = rope // 2
    hw = nope + rope
    width = heads * hw
    entry_w = lat + rope
    members = ranks * tp
    caches = (cache0, cache1)
    cache_b = (c_out0, c_out1)

    c = lax.axis_index("tp")
    d = lax.axis_index("dp")
    xx = lax.rem(d, SIDE)
    yy = lax.rem(d // SIDE, SIDE)
    pos = lax.rem(yy, 2) * 2 + lax.rem(xx, 2)
    corner = d - lax.rem(yy, 2) * SIDE - lax.rem(xx, 2)
    me = pos * tp + c

    def dp_of(q):
        return corner + (q // 2) * SIDE + lax.rem(q, 2)

    start = tiles_all * me // members
    count = tiles_all * (me + 1) // members - start
    base_tile = jnp.minimum(start, tiles_all - tiles)
    skip = start - base_tile
    first = pl.multiple_of(base_tile * LANES, LANES)

    qa_rows = w_qa.shape[1] // 2
    qb_rows = w_qb.shape[1] // 2
    o_rows = w_o.shape[1] // 4

    def attn_loads(layer):
        pairs = [("dkv", w_dkv.at[layer], dkv_b)]
        for i in range(2):
            cut = pl.ds(i * qa_rows, qa_rows)
            pairs.append((f"qa{i}", w_qa.at[layer, cut], qa_b.at[cut]))
        for i in range(2):
            cut = pl.ds(i * qb_rows, qb_rows)
            pairs.append((f"qb{i}", w_qb.at[layer, cut], qb_b.at[cut]))
        pairs.append(("uk", w_uk.at[layer], uk_b.at[:, pl.ds(0, nope), pl.ds(0, lat)]))
        for r in range(rows):
            pairs.append((f"c{r}", caches[layer].at[r], cache_b[layer].at[r]))
        pairs.append(("uv", w_uv.at[layer], uv_b))
        for i in range(4):
            cut = pl.ds(i * o_rows, o_rows)
            pairs.append((f"o{i}", w_o.at[layer, cut], o_b.at[cut]))
        loads = {name: pltpu.make_async_copy(a, b, a_sems.at[i]) for i, (name, a, b) in enumerate(pairs)}
        for load in loads.values():
            load.start()
        return loads

    def ffn_loads(layer):
        loads = [
            pltpu.make_async_copy(w_gate.at[layer, :, pl.ds(first, tiles * LANES)], gate_b, f_sems.at[0]),
            pltpu.make_async_copy(w_up.at[layer, :, pl.ds(first, tiles * LANES)], up_b, f_sems.at[1]),
            pltpu.make_async_copy(w_down.at[layer, pl.ds(first, tiles * LANES)], down_b, f_sems.at[2]),
        ]
        for load in loads:
            load.start()
        return loads

    a_loads = attn_loads(0)
    f_loads = ffn_loads(0)

    def peer(k):
        other = lax.rem(me + k, members)
        return other // tp, lax.rem(other, tp)

    barrier = pltpu.get_barrier_semaphore()
    for k in range(1, members):
        q, t = peer(k)
        pl.semaphore_signal(barrier, inc=1, device_id={"tp": t, "dp": dp_of(q)}, device_id_type=MESH)

    uk_b[:, nope:, :lat] = jnp.zeros((heads, rope, lat), BF16)
    sub = lax.broadcasted_iota(jnp.int32, (heads, hw, LANES), 1)
    lan = lax.broadcasted_iota(jnp.int32, (heads, hw, LANES), 2)
    uk_b[:, :, lat:] = jnp.where(sub == lan + nope, 1.0, 0.0).astype(BF16)
    entry_out[...] = jnp.zeros(entry_out.shape, F32)

    shape = (rows, period + LANES)
    row_id = lax.broadcasted_iota(jnp.int32, shape, 0)
    where_at = jnp.full(shape, len_ref[0].astype(F32))
    for r in range(1, rows):
        where_at = jnp.where(row_id == r, len_ref[r].astype(F32), where_at)
    turns = where_at * lane_ref[0:1, :]
    turns = (turns - jnp.floor(turns + 0.5)) + where_at * lane_ref[1:2, :]
    turns = turns - jnp.floor(turns + 0.5)
    cos_t, sin_t = cos_sin(turns)
    sin_t = sin_t * lane_ref[2:3, :]
    repeat = width // period
    cos_q = jnp.concatenate([cos_t[:, :period]] * repeat, axis=1)
    sin_q = jnp.concatenate([sin_t[:, :period]] * repeat, axis=1)
    cos_k, sin_k = cos_t[:, period:], sin_t[:, period:]
    sign_q = jnp.concatenate([jnp.broadcast_to(lane_ref[2:3, :period], (rows, period))] * repeat, axis=1)
    sign_k = jnp.broadcast_to(lane_ref[2:3, period:], (rows, LANES))

    spread_shape = (HEAD_PAD, width)
    head = lax.broadcasted_iota(jnp.int32, spread_shape, 0) * hw
    lane = lax.broadcasted_iota(jnp.int32, spread_shape, 1)
    spread_own = (lane >= head) & (lane < head + hw)
    v_dim = w_uv.shape[2]
    pick_shape = (HEAD_PAD, heads * v_dim)
    head = lax.broadcasted_iota(jnp.int32, pick_shape, 0) * v_dim
    lane = lax.broadcasted_iota(jnp.int32, pick_shape, 1)
    pick_own = (lane >= head) & (lane < head + v_dim)
    scale = hw ** -0.5
    x = x_ref[...].astype(F32)
    sends = []

    for layer in range(layers):
        cache = cache_b[layer]
        h = rms(x, attn_g[layer:layer + 1, :])
        a_loads["dkv"].wait()
        kv = dot_nt(h, dkv_b[...])
        k_lat = rms(kv[:, :lat], kv_g[layer:layer + 1, :])
        k_raw = jnp.concatenate([kv[:, lat:], jnp.zeros((rows, LANES - rope), F32)], axis=1)
        k_other = jnp.where(sign_k < 0, pltpu.roll(k_raw, LANES - half, 1), pltpu.roll(k_raw, half, 1))
        k_rot = (k_raw * cos_k + k_other * sin_k).astype(BF16)
        entry = jnp.concatenate([k_lat.astype(F32), k_rot.astype(F32)], axis=1)
        entry_out[layer * rows:(layer + 1) * rows, :] = entry

        qa = jnp.zeros((rows, w_qa.shape[2]), F32)
        for i in range(2):
            a_loads[f"qa{i}"].wait()
            qa += dot(h[:, i * qa_rows:(i + 1) * qa_rows], qa_b[pl.ds(i * qa_rows, qa_rows)])
        q_low = rms(qa, q_g[layer:layer + 1, :])
        q = jnp.zeros((rows, width), F32)
        for i in range(2):
            a_loads[f"qb{i}"].wait()
            q += dot(q_low[:, i * qb_rows:(i + 1) * qb_rows], qb_b[pl.ds(i * qb_rows, qb_rows)])
        q_other = jnp.where(sign_q < 0, pltpu.roll(q, width - half, 1), pltpu.roll(q, half, 1))
        q = q * cos_q + q_other * sin_q
        spread = jnp.concatenate([jnp.where(spread_own, jnp.broadcast_to(q[r:r + 1], spread_shape), 0.0) for r in range(rows)], axis=0).astype(BF16)
        a_loads["uk"].wait()
        query = dot(spread, uk_b[...].reshape(width, lat + LANES))

        o_lat = []
        for r in range(rows):
            a_loads[f"c{r}"].wait()
            length = len_ref[r]
            q_r = query[r * HEAD_PAD:(r + 1) * HEAD_PAD].astype(BF16)
            s_new = jnp.sum(q_r.astype(F32) * entry[r:r + 1], axis=1, keepdims=True) * scale
            top = s_new
            for k in range(slots // CHUNK):
                cols = pl.ds(k * CHUNK, CHUNK)
                s = dot(q_r[:, :lat], cache[r, pl.ds(0, lat), cols]) + dot(q_r[:, lat:entry_w], cache[r, pl.ds(lat, rope), cols])
                slot = lax.broadcasted_iota(jnp.int32, s.shape, 1) + k * CHUNK
                s = jnp.where(slot < length, s * scale, -1e30)
                s_b[r, :, cols] = s
                top = jnp.maximum(top, jnp.max(s, axis=1, keepdims=True))
            e_new = jnp.exp(s_new - top)
            total = e_new
            for k in range(slots // CHUNK):
                cols = pl.ds(k * CHUNK, CHUNK)
                e = jnp.exp(s_b[r, :, cols] - top)
                s_b[r, :, cols] = e
                total += jnp.sum(e, axis=1, keepdims=True)
            inv = 1.0 / total
            acc = (e_new * inv).astype(BF16).astype(F32) * entry[r:r + 1, :lat]
            for k in range(slots // CHUNK):
                cols = pl.ds(k * CHUNK, CHUNK)
                p = (s_b[r, :, cols] * inv).astype(BF16)
                acc += dot_nt(p, cache[r, pl.ds(0, lat), cols])
            o_lat.append(acc)
        o_lat = jnp.concatenate(o_lat, axis=0).astype(BF16)
        a_loads["uv"].wait()
        wide = dot_nt(o_lat, uv_b[...].reshape(heads * v_dim, lat))
        o = [jnp.sum(jnp.where(pick_own, wide[r * HEAD_PAD:(r + 1) * HEAD_PAD], 0.0), axis=0, keepdims=True) for r in range(rows)]
        o = jnp.concatenate(o, axis=0).astype(BF16)
        part = x * jnp.where(c == 0, 1.0, 0.0)
        for i in range(4):
            a_loads[f"o{i}"].wait()
            part += dot(o[:, i * o_rows:(i + 1) * o_rows], o_b[pl.ds(i * o_rows, o_rows)])

        mine_b[layer] = part
        if layer == 0:
            pl.semaphore_wait(barrier, members - 1)
        swap = pltpu.make_async_remote_copy(
            src_ref=mine_b.at[layer], dst_ref=part_b.at[layer], send_sem=ps.at[layer], recv_sem=pr.at[layer],
            device_id={"tp": 1 - c, "dp": d}, device_id_type=MESH)
        swap.start()
        if layer + 1 < layers:
            a_loads = attn_loads(layer + 1)
        swap.wait_recv()
        x_mid = (part + part_b[layer]).astype(BF16)
        mid_b[layer, pos] = x_mid

        gathers = []
        for k in range(1, ranks):
            q = lax.rem(pos + k, ranks)
            for t in range(tp):
                gathers.append(pltpu.make_async_remote_copy(
                    src_ref=mid_b.at[layer, pos], dst_ref=mid_b.at[layer, pos], send_sem=ms.at[layer, k - 1, t], recv_sem=mr.at[layer, k - 1],
                    device_id={"tp": t, "dp": dp_of(q)}, device_id_type=MESH))

        @pl.when(c == tp - 1)
        def _():
            for copy in gathers:
                copy.start()
        for k in range(ranks - 1):
            gathers[k * tp].wait_recv()

        for q in range(ranks):
            all_b[q * rows:(q + 1) * rows, :] = mid_b[layer, q].astype(F32)
        g = rms(all_b[...], ffn_g[layer:layer + 1, :])
        f_loads[0].wait()
        a = dot(g, gate_b[...])
        f_loads[1].wait()
        b = dot(g, up_b[...])
        lane = lax.broadcasted_iota(jnp.int32, a.shape, 1)
        kept = (lane >= skip * LANES) & (lane < (skip + count) * LANES)
        u = jnp.where(kept, a * jax.nn.sigmoid(a) * b, 0.0).astype(BF16)
        f_loads[2].wait()
        partial = dot(u, down_b[...])
        for q in range(ranks):
            send_b[layer, q] = partial[q * rows:(q + 1) * rows].astype(BF16)
        sum_b[layer, me] = send_b[layer, pos]

        returns = []
        for k in range(1, members):
            q, t = peer(k)
            returns.append(pltpu.make_async_remote_copy(
                src_ref=send_b.at[layer, q], dst_ref=sum_b.at[layer, me], send_sem=rs.at[layer, k - 1], recv_sem=rr.at[layer, k - 1],
                device_id={"tp": t, "dp": dp_of(q)}, device_id_type=MESH))
        for copy in returns:
            copy.start()
        if layer + 1 < layers:
            f_loads = ffn_loads(layer + 1)
        for copy in returns:
            copy.wait_recv()
        total = sum_b[layer, 0].astype(F32)
        for j in range(1, members):
            total = total + sum_b[layer, j].astype(F32)
        x_new = (x_mid.astype(F32) + total).astype(BF16)
        x = x_new.astype(F32)
        sends.append((swap, gathers, returns))

    x_out[...] = x_new
    for swap, gathers, returns in sends:
        swap.wait_send()
        for copy in returns:
            copy.wait_send()

        @pl.when(c == tp - 1)
        def _():
            for copy in gathers:
                copy.wait_send()


def write_kernel(dims, len_ref, x_ref, entry_ref, c0, c1, x_out, out0, out1, patch_b, sems):
    layers, rows, entry_w, slots = dims
    x_out[...] = x_ref[...]
    entry_t = entry_ref[...].T[:entry_w]
    caches, outs = (c0, c1), (out0, out1)
    for layer in range(layers):
        for r in range(rows):
            length = len_ref[r]
            home = length // OUT_CHUNK
            for k in range(slots // OUT_CHUNK):
                cols = pl.ds(k * OUT_CHUNK, OUT_CHUNK)

                @pl.when(home != k)
                def _():
                    pltpu.make_async_copy(caches[layer].at[r, :, cols], outs[layer].at[r, :, cols], sems.at[layer, r]).start()
    for layer in range(layers):
        for r in range(rows):
            length = len_ref[r]
            base = pl.multiple_of(length // OUT_CHUNK * OUT_CHUNK, OUT_CHUNK)
            tile = caches[layer][r, :, pl.ds(base, OUT_CHUNK)].astype(F32)
            lane = lax.broadcasted_iota(jnp.int32, tile.shape, 1)
            column = entry_t[:, layer * rows + r:layer * rows + r + 1]
            patch_b[layer, r] = jnp.where(lane == length - base, jnp.broadcast_to(column, tile.shape), tile).astype(BF16)
            pltpu.make_async_copy(patch_b.at[layer, r], outs[layer].at[r, :, pl.ds(base, OUT_CHUNK)], sems.at[layer, r]).start()
    for layer in range(layers):
        for r in range(rows):
            pltpu.make_async_copy(caches[layer].at[r], outs[layer].at[r], sems.at[layer, r]).wait()


def solution(mesh):
    tp_size = mesh.shape['tp']
    ranks = 4
    row_spec = P(('rep', 'dp'), None)
    cache_spec = P(('rep', 'dp'), None, None)
    in_specs = (row_spec, P(('rep', 'dp')), cache_spec, cache_spec, P(), P(), P(), P(), P(), P(), P(None, None, 'tp'), P(None, 'tp', None, None), P(None, 'tp', None, None), P(None, 'tp', None), P(), P(), P())
    out_specs = (row_spec, cache_spec, cache_spec)

    def local_step(x, lengths, cache0, cache1, attn_gain, kv_gain, q_gain, ffn_gain, w_dkv, w_qa, w_qb, w_uk, w_uv, w_o, w_gate, w_up, w_down):
        rows, model = x.shape
        layers, heads, nope, lat = w_uk.shape
        slots = cache0.shape[1]
        rope = cache0.shape[2] - lat
        hw = nope + rope
        period = int(np.lcm(hw, LANES))
        tiles_all = w_gate.shape[2] // LANES
        members = ranks * tp_size
        tiles = -(-tiles_all // members)
        lanes = jnp.asarray(rope_lanes(hw, nope, rope, period))
        c0, c1 = jnp.swapaxes(cache0, 1, 2), jnp.swapaxes(cache1, 1, 2)
        w_dkv_t = jnp.swapaxes(w_dkv, 1, 2)
        w_uv_t = jnp.swapaxes(w_uv, 2, 3)
        dims = (layers, rows, heads, nope, rope, lat, slots, tiles_all, tiles, ranks, tp_size, period)
        dma = pltpu.SemaphoreType.DMA
        x_new, entries, held0, held1 = pl.pallas_call(
            functools.partial(step_kernel, dims),
            name="step",
            out_shape=(pltpu.VMEM((rows, model), BF16), pltpu.VMEM((8, lat + LANES), F32), pltpu.VMEM(c0.shape, BF16), pltpu.VMEM(c1.shape, BF16)),
            in_specs=[SMEM_SPEC] + [VMEM_SPEC] * 6 + [HBM_SPEC] * 11,
            out_specs=(VMEM_SPEC, VMEM_SPEC, VMEM_SPEC, VMEM_SPEC),
            scratch_shapes=[
                pltpu.VMEM(w_dkv_t.shape[1:], BF16),
                pltpu.VMEM(w_qa.shape[1:], BF16),
                pltpu.VMEM(w_qb.shape[1:], BF16),
                pltpu.VMEM((heads, hw, lat + LANES), BF16),
                pltpu.VMEM(w_uv_t.shape[1:], BF16),
                pltpu.VMEM(w_o.shape[1:], BF16),
                pltpu.VMEM((model, tiles * LANES), BF16),
                pltpu.VMEM((model, tiles * LANES), BF16),
                pltpu.VMEM((tiles * LANES, model), BF16),
                pltpu.VMEM((rows, HEAD_PAD, slots), F32),
                pltpu.VMEM((layers, rows, model), F32),
                pltpu.VMEM((layers, rows, model), F32),
                pltpu.VMEM((layers, ranks, rows, model), BF16),
                pltpu.VMEM((ranks * rows, model), F32),
                pltpu.VMEM((layers, ranks, rows, model), BF16),
                pltpu.VMEM((layers, members, rows, model), BF16),
                dma((13,)),
                dma((3,)),
                dma((layers,)),
                dma((layers,)),
                dma((layers, ranks - 1, tp_size)),
                dma((layers, ranks - 1)),
                dma((layers, members - 1)),
                dma((layers, members - 1)),
            ],
            compiler_params=pltpu.CompilerParams(collective_id=0, has_side_effects=True, vmem_limit_bytes=46 * 2 ** 20),
            cost_estimate=pl.CostEstimate(flops=10 ** 9, bytes_accessed=70 * 10 ** 6, transcendentals=4 * 10 ** 5),
        )(lengths, lanes, x, attn_gain, kv_gain, q_gain, ffn_gain, c0, c1, w_dkv_t, w_qa, w_qb, w_uk, w_uv_t, w_o, w_gate, w_up, w_down)
        x_new, new0, new1 = pl.pallas_call(
            functools.partial(write_kernel, (layers, rows, lat + rope, slots)),
            name="write",
            out_shape=(jax.ShapeDtypeStruct(x.shape, BF16), jax.ShapeDtypeStruct(c0.shape, BF16), jax.ShapeDtypeStruct(c1.shape, BF16)),
            in_specs=[SMEM_SPEC, VMEM_SPEC, VMEM_SPEC, VMEM_SPEC, VMEM_SPEC],
            out_specs=(VMEM_SPEC, HBM_SPEC, HBM_SPEC),
            scratch_shapes=[pltpu.VMEM((layers, rows, lat + rope, OUT_CHUNK), BF16), dma((layers, rows))],
            compiler_params=pltpu.CompilerParams(vmem_limit_bytes=24 * 2 ** 20),
            cost_estimate=pl.CostEstimate(flops=10 ** 6, bytes_accessed=20 * 10 ** 6, transcendentals=0),
        )(lengths, x_new, entries, held0, held1)
        return x_new, jnp.swapaxes(new0, 1, 2), jnp.swapaxes(new1, 1, 2)

    return jax.shard_map(local_step, mesh=mesh, in_specs=in_specs, out_specs=out_specs, check_vma=False)
```

```python
import functools

import jax
import jax.numpy as jnp
import numpy as np
from jax import lax
from jax.experimental import pallas as pl
from jax.experimental.pallas import tpu as pltpu
from jax.sharding import PartitionSpec as P

MESH = pl.DeviceIdType.MESH
NORM_EPS = 1e-6
ROPE_BASE = 10000.0
HEAD_PAD = 24
LANES = 128
PASS = 256
CHUNK = 1024
OUT_CHUNK = 512
SIDE = 4
VMEM_SPEC = pl.BlockSpec(memory_space=pltpu.VMEM)
SMEM_SPEC = pl.BlockSpec(memory_space=pltpu.SMEM)
HBM_SPEC = pl.BlockSpec(memory_space=pltpu.HBM)
NT = (((1,), (1,)), ((), ()))
F32 = jnp.float32
BF16 = jnp.bfloat16


def dot(a, b):
    return jnp.dot(a, b, preferred_element_type=F32)


def dot_nt(a, b):
    return lax.dot_general(a, b, NT, preferred_element_type=F32)


def rms(values, gain):
    inv = lax.rsqrt(jnp.mean(values * values, axis=-1, keepdims=True) + NORM_EPS)
    return (values * inv * gain).astype(BF16)


def rope_lanes(head_width, nope, rope, period):
    half = rope // 2
    turns = ROPE_BASE ** (-2.0 * np.arange(half) / rope) / (2.0 * np.pi)
    freq = np.zeros(period + LANES)
    sign = np.zeros(period + LANES)
    for s in [h * head_width + nope for h in range(period // head_width)] + [period]:
        freq[s:s + half] = turns
        freq[s + half:s + rope] = turns
        sign[s:s + half] = -1.0
        sign[s + half:s + rope] = 1.0
    mant, expo = np.frexp(freq)
    high = np.ldexp(np.floor(mant * 2.0 ** 12), expo - 12)
    table = np.zeros((8, period + LANES), np.float32)
    table[0], table[1], table[2] = high, freq - high, sign
    return table


def cuts(size, count):
    step = size // count // PASS * PASS
    starts = [i * step for i in range(count)]
    return [(a, b - a) for a, b in zip(starts, starts[1:] + [size])]


def series(x, terms):
    out = jnp.full(x.shape, terms[-1], F32)
    for t in terms[-2::-1]:
        out = out * x + t
    return out


def cos_sin(turns):
    x = turns * np.float32(np.pi)
    x2 = x * x
    fact = np.cumprod([1.0] + list(range(1, 18)))
    s = x * series(x2, [np.float32((-1.0) ** i / fact[2 * i + 1]) for i in range(8)])
    c = series(x2, [np.float32((-1.0) ** i / fact[2 * i]) for i in range(9)])
    return 1.0 - 2.0 * s * s, 2.0 * s * c


def step_kernel(dims, len_ref, lane_ref, x_ref, attn_g, kv_g, q_g, ffn_g, cache0, cache1, w_dkv, w_qa, w_qb, w_uk, w_uv, w_o, w_gate, w_up, w_down,
                x_out, entry_out, c_out0, c_out1,
                dkv_b, qa_b, qb_b, uk_b, uv_b, o_b, gate_b, up_b, down_b, s_b, mine_b, part_b, mid_b, all_b, send_b, sum_b,
                a_sems, f_sems, ps, pr, ms, mr, rs, rr):
    layers, rows, heads, nope, rope, lat, slots, tiles_all, tiles, ranks, tp, period = dims
    half = rope // 2
    hw = nope + rope
    width = heads * hw
    entry_w = lat + rope
    members = ranks * tp
    caches = (cache0, cache1)
    cache_b = (c_out0, c_out1)

    c = lax.axis_index("tp")
    d = lax.axis_index("dp")
    xx = lax.rem(d, SIDE)
    yy = lax.rem(d // SIDE, SIDE)
    pos = lax.rem(yy, 2) * 2 + lax.rem(xx, 2)
    corner = d - lax.rem(yy, 2) * SIDE - lax.rem(xx, 2)
    me = pos * tp + c

    def dp_of(q):
        return corner + (q // 2) * SIDE + lax.rem(q, 2)

    start = tiles_all * me // members
    count = tiles_all * (me + 1) // members - start
    base_tile = jnp.minimum(start, tiles_all - tiles)
    skip = start - base_tile
    first = pl.multiple_of(base_tile * LANES, LANES)

    qa_rows = w_qa.shape[1] // 2
    o_cuts = cuts(w_o.shape[1], 2)

    def attn_loads(layer):
        pairs = [("dkv", w_dkv.at[layer], dkv_b)]
        for i in range(2):
            cut = pl.ds(i * qa_rows, qa_rows)
            pairs.append((f"qa{i}", w_qa.at[layer, cut], qa_b.at[cut]))
        pairs.append(("qb", w_qb.at[layer], qb_b))
        pairs.append(("uk", w_uk.at[layer], uk_b.at[:, pl.ds(0, nope), pl.ds(0, lat)]))
        for r in range(rows):
            pairs.append((f"c{r}", caches[layer].at[r], cache_b[layer].at[r]))
        pairs.append(("uv", w_uv.at[layer], uv_b))
        for i, (at, size) in enumerate(o_cuts):
            cut = pl.ds(at, size)
            pairs.append((f"o{i}", w_o.at[layer, cut], o_b.at[cut]))
        loads = {name: pltpu.make_async_copy(a, b, a_sems.at[i]) for i, (name, a, b) in enumerate(pairs)}
        for load in loads.values():
            load.start()
        return loads

    def ffn_loads(layer):
        loads = [
            pltpu.make_async_copy(w_gate.at[layer, :, pl.ds(first, tiles * LANES)], gate_b, f_sems.at[0]),
            pltpu.make_async_copy(w_up.at[layer, :, pl.ds(first, tiles * LANES)], up_b, f_sems.at[1]),
            pltpu.make_async_copy(w_down.at[layer, pl.ds(first, tiles * LANES)], down_b, f_sems.at[2]),
        ]
        for load in loads:
            load.start()
        return loads

    a_loads = attn_loads(0)
    f_loads = ffn_loads(0)

    def peer(k):
        other = lax.rem(me + k, members)
        return other // tp, lax.rem(other, tp)

    barrier = pltpu.get_barrier_semaphore()
    for k in range(1, members):
        q, t = peer(k)
        pl.semaphore_signal(barrier, inc=1, device_id={"tp": t, "dp": dp_of(q)}, device_id_type=MESH)

    uk_b[:, nope:, :lat] = jnp.zeros((heads, rope, lat), BF16)
    sub = lax.broadcasted_iota(jnp.int32, (heads, hw, LANES), 1)
    lan = lax.broadcasted_iota(jnp.int32, (heads, hw, LANES), 2)
    uk_b[:, :, lat:] = jnp.where(sub == lan + nope, 1.0, 0.0).astype(BF16)
    entry_out[...] = jnp.zeros(entry_out.shape, F32)

    shape = (rows, period + LANES)
    row_id = lax.broadcasted_iota(jnp.int32, shape, 0)
    where_at = jnp.full(shape, len_ref[0].astype(F32))
    for r in range(1, rows):
        where_at = jnp.where(row_id == r, len_ref[r].astype(F32), where_at)
    turns = where_at * lane_ref[0:1, :]
    turns = (turns - jnp.floor(turns + 0.5)) + where_at * lane_ref[1:2, :]
    turns = turns - jnp.floor(turns + 0.5)
    cos_t, sin_t = cos_sin(turns)
    sin_t = sin_t * lane_ref[2:3, :]
    repeat = width // period
    cos_q = jnp.concatenate([cos_t[:, :period]] * repeat, axis=1)
    sin_q = jnp.concatenate([sin_t[:, :period]] * repeat, axis=1)
    cos_k, sin_k = cos_t[:, period:], sin_t[:, period:]
    sign_q = jnp.concatenate([jnp.broadcast_to(lane_ref[2:3, :period], (rows, period))] * repeat, axis=1)
    sign_k = jnp.broadcast_to(lane_ref[2:3, period:], (rows, LANES))

    spread_shape = (HEAD_PAD, width)
    head = lax.broadcasted_iota(jnp.int32, spread_shape, 0) * hw
    lane = lax.broadcasted_iota(jnp.int32, spread_shape, 1)
    spread_own = (lane >= head) & (lane < head + hw)
    v_dim = w_uv.shape[2]
    pick_shape = (HEAD_PAD, heads * v_dim)
    head = lax.broadcasted_iota(jnp.int32, pick_shape, 0) * v_dim
    lane = lax.broadcasted_iota(jnp.int32, pick_shape, 1)
    pick_own = (lane >= head) & (lane < head + v_dim)
    scale = hw ** -0.5
    x = x_ref[...].astype(F32)
    sends = []

    for layer in range(layers):
        cache = cache_b[layer]
        h = rms(x, attn_g[layer:layer + 1, :])
        a_loads["dkv"].wait()
        kv = dot_nt(h, dkv_b[...])
        k_lat = rms(kv[:, :lat], kv_g[layer:layer + 1, :])
        k_raw = jnp.concatenate([kv[:, lat:], jnp.zeros((rows, LANES - rope), F32)], axis=1)
        k_other = jnp.where(sign_k < 0, pltpu.roll(k_raw, LANES - half, 1), pltpu.roll(k_raw, half, 1))
        k_rot = (k_raw * cos_k + k_other * sin_k).astype(BF16)
        entry = jnp.concatenate([k_lat.astype(F32), k_rot.astype(F32)], axis=1)
        entry_out[layer * rows:(layer + 1) * rows, :] = entry

        qa = jnp.zeros((rows, w_qa.shape[2]), F32)
        for i in range(2):
            a_loads[f"qa{i}"].wait()
            qa += dot(h[:, i * qa_rows:(i + 1) * qa_rows], qa_b[pl.ds(i * qa_rows, qa_rows)])
        q_low = rms(qa, q_g[layer:layer + 1, :])
        a_loads["qb"].wait()
        q = dot(q_low, qb_b[...])
        q_other = jnp.where(sign_q < 0, pltpu.roll(q, width - half, 1), pltpu.roll(q, half, 1))
        q = q * cos_q + q_other * sin_q
        spread = jnp.concatenate([jnp.where(spread_own, jnp.broadcast_to(q[r:r + 1], spread_shape), 0.0) for r in range(rows)], axis=0).astype(BF16)
        a_loads["uk"].wait()
        query = dot(spread, uk_b[...].reshape(width, lat + LANES))

        tail = query[:, lat:]
        group = lax.broadcasted_iota(jnp.int32, tail.shape, 0)
        rotary = tail
        for r in range(1, rows):
            rotary = jnp.where(group >= r * HEAD_PAD, pltpu.roll(tail, r * rope, 1), rotary)
        rotary = rotary[:, :rows * rope].astype(BF16)
        q_rows = [query[r * HEAD_PAD:(r + 1) * HEAD_PAD].astype(BF16) for r in range(rows)]
        s_new = [jnp.sum(q_rows[r].astype(F32) * entry[r:r + 1], axis=1, keepdims=True) * scale for r in range(rows)]
        top = list(s_new)
        for r in range(rows):
            a_loads[f"c{r}"].wait()
        for k in range(slots // CHUNK):
            cols = pl.ds(k * CHUNK, CHUNK)
            stacked = jnp.concatenate([cache[r, pl.ds(lat, rope), cols] for r in range(rows)], axis=0)
            s_rot = dot(rotary, stacked)
            for r in range(rows):
                s = dot(q_rows[r][:, :lat], cache[r, pl.ds(0, lat), cols]) + s_rot[r * HEAD_PAD:(r + 1) * HEAD_PAD]
                slot = lax.broadcasted_iota(jnp.int32, s.shape, 1) + k * CHUNK
                s = jnp.where(slot < len_ref[r], s * scale, -1e30)
                s_b[r, :, cols] = s
                top[r] = jnp.maximum(top[r], jnp.max(s, axis=1, keepdims=True))
        o_lat = []
        for r in range(rows):
            e_new = jnp.exp(s_new[r] - top[r])
            total = e_new
            for k in range(slots // CHUNK):
                cols = pl.ds(k * CHUNK, CHUNK)
                e = jnp.exp(s_b[r, :, cols] - top[r])
                s_b[r, :, cols] = e
                total += jnp.sum(e, axis=1, keepdims=True)
            inv = 1.0 / total
            acc = (e_new * inv).astype(BF16).astype(F32) * entry[r:r + 1, :lat]
            for k in range(slots // CHUNK):
                cols = pl.ds(k * CHUNK, CHUNK)
                p = (s_b[r, :, cols] * inv).astype(BF16)
                acc += dot_nt(p, cache[r, pl.ds(0, lat), cols])
            o_lat.append(acc)
        o_lat = jnp.concatenate(o_lat, axis=0).astype(BF16)
        a_loads["uv"].wait()
        wide = dot_nt(o_lat, uv_b[...].reshape(heads * v_dim, lat))
        o = [jnp.sum(jnp.where(pick_own, wide[r * HEAD_PAD:(r + 1) * HEAD_PAD], 0.0), axis=0, keepdims=True) for r in range(rows)]
        o = jnp.concatenate(o, axis=0).astype(BF16)
        part = x * jnp.where(c == 0, 1.0, 0.0)
        for i, (at, size) in enumerate(o_cuts):
            a_loads[f"o{i}"].wait()
            part += dot(o[:, at:at + size], o_b[pl.ds(at, size)])

        mine_b[layer] = part
        if layer == 0:
            pl.semaphore_wait(barrier, members - 1)
        swap = pltpu.make_async_remote_copy(
            src_ref=mine_b.at[layer], dst_ref=part_b.at[layer], send_sem=ps.at[layer], recv_sem=pr.at[layer],
            device_id={"tp": 1 - c, "dp": d}, device_id_type=MESH)
        swap.start()
        if layer + 1 < layers:
            a_loads = attn_loads(layer + 1)
        swap.wait_recv()
        x_mid = (part + part_b[layer]).astype(BF16)
        mid_b[layer, pos] = x_mid

        gathers = []
        for k in range(1, ranks):
            q = lax.rem(pos + k, ranks)
            for t in range(tp):
                gathers.append(pltpu.make_async_remote_copy(
                    src_ref=mid_b.at[layer, pos], dst_ref=mid_b.at[layer, pos], send_sem=ms.at[layer, k - 1, t], recv_sem=mr.at[layer, k - 1],
                    device_id={"tp": t, "dp": dp_of(q)}, device_id_type=MESH))

        @pl.when(c == tp - 1)
        def _():
            for copy in gathers:
                copy.start()
        for k in range(ranks - 1):
            gathers[k * tp].wait_recv()

        for q in range(ranks):
            all_b[q * rows:(q + 1) * rows, :] = mid_b[layer, q].astype(F32)
        g = rms(all_b[...], ffn_g[layer:layer + 1, :])
        f_loads[0].wait()
        whole = tiles * LANES // PASS * PASS
        a = dot(g, gate_b[:, :whole])
        f_loads[1].wait()
        b = dot(g, up_b[:, :whole])
        if whole < tiles * LANES:
            both = dot(g, jnp.concatenate([gate_b[:, whole:], up_b[:, whole:]], axis=1))
            a = jnp.concatenate([a, both[:, :LANES]], axis=1)
            b = jnp.concatenate([b, both[:, LANES:]], axis=1)
        lane = lax.broadcasted_iota(jnp.int32, a.shape, 1)
        kept = (lane >= skip * LANES) & (lane < (skip + count) * LANES)
        u = jnp.where(kept, a * jax.nn.sigmoid(a) * b, 0.0).astype(BF16)
        f_loads[2].wait()
        partial = dot(u, down_b[...])
        for q in range(ranks):
            send_b[layer, q] = partial[q * rows:(q + 1) * rows].astype(BF16)
        sum_b[layer, me] = send_b[layer, pos]

        returns = []
        for k in range(1, members):
            q, t = peer(k)
            returns.append(pltpu.make_async_remote_copy(
                src_ref=send_b.at[layer, q], dst_ref=sum_b.at[layer, me], send_sem=rs.at[layer, k - 1], recv_sem=rr.at[layer, k - 1],
                device_id={"tp": t, "dp": dp_of(q)}, device_id_type=MESH))
        for copy in returns:
            copy.start()
        if layer + 1 < layers:
            f_loads = ffn_loads(layer + 1)
        for copy in returns:
            copy.wait_recv()
        total = sum_b[layer, 0].astype(F32)
        for j in range(1, members):
            total = total + sum_b[layer, j].astype(F32)
        x_new = (x_mid.astype(F32) + total).astype(BF16)
        x = x_new.astype(F32)
        sends.append((swap, gathers, returns))

    x_out[...] = x_new
    for swap, gathers, returns in sends:
        swap.wait_send()
        for copy in returns:
            copy.wait_send()

        @pl.when(c == tp - 1)
        def _():
            for copy in gathers:
                copy.wait_send()


def write_kernel(dims, len_ref, x_ref, entry_ref, c0, c1, x_out, out0, out1, patch_b, x_sem, sems):
    layers, rows, entry_w, slots = dims
    x_copy = pltpu.make_async_copy(x_ref, x_out, x_sem.at[0])
    x_copy.start()
    entry_t = entry_ref[...].T[:entry_w]
    caches, outs = (c0, c1), (out0, out1)
    for layer in range(layers):
        for r in range(rows):
            length = len_ref[r]
            home = length // OUT_CHUNK
            for k in range(slots // OUT_CHUNK):
                cols = pl.ds(k * OUT_CHUNK, OUT_CHUNK)

                @pl.when(home != k)
                def _():
                    pltpu.make_async_copy(caches[layer].at[r, :, cols], outs[layer].at[r, :, cols], sems.at[layer, r]).start()
    for layer in range(layers):
        for r in range(rows):
            length = len_ref[r]
            base = pl.multiple_of(length // OUT_CHUNK * OUT_CHUNK, OUT_CHUNK)
            tile = caches[layer][r, :, pl.ds(base, OUT_CHUNK)].astype(F32)
            lane = lax.broadcasted_iota(jnp.int32, tile.shape, 1)
            column = entry_t[:, layer * rows + r:layer * rows + r + 1]
            patch_b[layer, r] = jnp.where(lane == length - base, jnp.broadcast_to(column, tile.shape), tile).astype(BF16)
            pltpu.make_async_copy(patch_b.at[layer, r], outs[layer].at[r, :, pl.ds(base, OUT_CHUNK)], sems.at[layer, r]).start()
    for layer in range(layers):
        for r in range(rows):
            pltpu.make_async_copy(caches[layer].at[r], outs[layer].at[r], sems.at[layer, r]).wait()
    x_copy.wait()


def solution(mesh):
    tp_size = mesh.shape['tp']
    ranks = 4
    row_spec = P(('rep', 'dp'), None)
    cache_spec = P(('rep', 'dp'), None, None)
    in_specs = (row_spec, P(('rep', 'dp')), cache_spec, cache_spec, P(), P(), P(), P(), P(), P(), P(None, None, 'tp'), P(None, 'tp', None, None), P(None, 'tp', None, None), P(None, 'tp', None), P(), P(), P())
    out_specs = (row_spec, cache_spec, cache_spec)

    def local_step(x, lengths, cache0, cache1, attn_gain, kv_gain, q_gain, ffn_gain, w_dkv, w_qa, w_qb, w_uk, w_uv, w_o, w_gate, w_up, w_down):
        rows, model = x.shape
        layers, heads, nope, lat = w_uk.shape
        slots = cache0.shape[1]
        rope = cache0.shape[2] - lat
        hw = nope + rope
        period = int(np.lcm(hw, LANES))
        tiles_all = w_gate.shape[2] // LANES
        members = ranks * tp_size
        tiles = -(-tiles_all // members)
        lanes = jnp.asarray(rope_lanes(hw, nope, rope, period))
        c0, c1 = jnp.swapaxes(cache0, 1, 2), jnp.swapaxes(cache1, 1, 2)
        w_dkv_t = jnp.swapaxes(w_dkv, 1, 2)
        w_uv_t = jnp.swapaxes(w_uv, 2, 3)
        dims = (layers, rows, heads, nope, rope, lat, slots, tiles_all, tiles, ranks, tp_size, period)
        dma = pltpu.SemaphoreType.DMA
        x_new, entries, held0, held1 = pl.pallas_call(
            functools.partial(step_kernel, dims),
            name="step",
            out_shape=(pltpu.VMEM((rows, model), BF16), pltpu.VMEM((8, lat + LANES), F32), pltpu.VMEM(c0.shape, BF16), pltpu.VMEM(c1.shape, BF16)),
            in_specs=[SMEM_SPEC] + [VMEM_SPEC] * 6 + [HBM_SPEC] * 11,
            out_specs=(VMEM_SPEC, VMEM_SPEC, VMEM_SPEC, VMEM_SPEC),
            scratch_shapes=[
                pltpu.VMEM(w_dkv_t.shape[1:], BF16),
                pltpu.VMEM(w_qa.shape[1:], BF16),
                pltpu.VMEM(w_qb.shape[1:], BF16),
                pltpu.VMEM((heads, hw, lat + LANES), BF16),
                pltpu.VMEM(w_uv_t.shape[1:], BF16),
                pltpu.VMEM(w_o.shape[1:], BF16),
                pltpu.VMEM((model, tiles * LANES), BF16),
                pltpu.VMEM((model, tiles * LANES), BF16),
                pltpu.VMEM((tiles * LANES, model), BF16),
                pltpu.VMEM((rows, HEAD_PAD, slots), F32),
                pltpu.VMEM((layers, rows, model), F32),
                pltpu.VMEM((layers, rows, model), F32),
                pltpu.VMEM((layers, ranks, rows, model), BF16),
                pltpu.VMEM((ranks * rows, model), F32),
                pltpu.VMEM((layers, ranks, rows, model), BF16),
                pltpu.VMEM((layers, members, rows, model), BF16),
                dma((10,)),
                dma((3,)),
                dma((layers,)),
                dma((layers,)),
                dma((layers, ranks - 1, tp_size)),
                dma((layers, ranks - 1)),
                dma((layers, members - 1)),
                dma((layers, members - 1)),
            ],
            compiler_params=pltpu.CompilerParams(collective_id=0, has_side_effects=True, vmem_limit_bytes=46 * 2 ** 20),
            cost_estimate=pl.CostEstimate(flops=10 ** 9, bytes_accessed=70 * 10 ** 6, transcendentals=4 * 10 ** 5),
        )(lengths, lanes, x, attn_gain, kv_gain, q_gain, ffn_gain, c0, c1, w_dkv_t, w_qa, w_qb, w_uk, w_uv_t, w_o, w_gate, w_up, w_down)
        x_new, new0, new1 = pl.pallas_call(
            functools.partial(write_kernel, (layers, rows, lat + rope, slots)),
            name="write",
            out_shape=(jax.ShapeDtypeStruct(x.shape, BF16), jax.ShapeDtypeStruct(c0.shape, BF16), jax.ShapeDtypeStruct(c1.shape, BF16)),
            in_specs=[SMEM_SPEC, VMEM_SPEC, VMEM_SPEC, VMEM_SPEC, VMEM_SPEC],
            out_specs=(HBM_SPEC, HBM_SPEC, HBM_SPEC),
            scratch_shapes=[pltpu.VMEM((layers, rows, lat + rope, OUT_CHUNK), BF16), dma((1,)), dma((layers, rows))],
            compiler_params=pltpu.CompilerParams(vmem_limit_bytes=24 * 2 ** 20),
            cost_estimate=pl.CostEstimate(flops=10 ** 6, bytes_accessed=20 * 10 ** 6, transcendentals=0),
        )(lengths, x_new, entries, held0, held1)
        return x_new, jnp.swapaxes(new0, 1, 2), jnp.swapaxes(new1, 1, 2)

    return jax.shard_map(local_step, mesh=mesh, in_specs=in_specs, out_specs=out_specs, check_vma=False)
```

```python
import functools

import jax
import jax.numpy as jnp
import numpy as np
from jax import lax
from jax.experimental import pallas as pl
from jax.experimental.pallas import tpu as pltpu
from jax.sharding import PartitionSpec as P

MESH = pl.DeviceIdType.MESH
NORM_EPS = 1e-6
ROPE_BASE = 10000.0
HEAD_PAD = 24
LANES = 128
PASS = 256
CHUNK = 1024
OUT_CHUNK = 512
SIDE = 4
VMEM_SPEC = pl.BlockSpec(memory_space=pltpu.VMEM)
SMEM_SPEC = pl.BlockSpec(memory_space=pltpu.SMEM)
HBM_SPEC = pl.BlockSpec(memory_space=pltpu.HBM)
NT = (((1,), (1,)), ((), ()))
F32 = jnp.float32
BF16 = jnp.bfloat16


def dot(a, b):
    return jnp.dot(a, b, preferred_element_type=F32)


def dot_nt(a, b):
    return lax.dot_general(a, b, NT, preferred_element_type=F32)


def rms(values, gain):
    inv = lax.rsqrt(jnp.mean(values * values, axis=-1, keepdims=True) + NORM_EPS)
    return (values * inv * gain).astype(BF16)


def rope_lanes(head_width, nope, rope, period):
    half = rope // 2
    turns = ROPE_BASE ** (-2.0 * np.arange(half) / rope) / (2.0 * np.pi)
    freq = np.zeros(period + LANES)
    sign = np.zeros(period + LANES)
    for s in [h * head_width + nope for h in range(period // head_width)] + [period]:
        freq[s:s + half] = turns
        freq[s + half:s + rope] = turns
        sign[s:s + half] = -1.0
        sign[s + half:s + rope] = 1.0
    mant, expo = np.frexp(freq)
    high = np.ldexp(np.floor(mant * 2.0 ** 12), expo - 12)
    table = np.zeros((8, period + LANES), np.float32)
    table[0], table[1], table[2] = high, freq - high, sign
    return table


def cuts(size, count):
    step = size // count // PASS * PASS
    starts = [i * step for i in range(count)]
    return [(a, b - a) for a, b in zip(starts, starts[1:] + [size])]


def series(x, terms):
    out = jnp.full(x.shape, terms[-1], F32)
    for t in terms[-2::-1]:
        out = out * x + t
    return out


def cos_sin(turns):
    x = turns * np.float32(np.pi)
    x2 = x * x
    fact = np.cumprod([1.0] + list(range(1, 18)))
    s = x * series(x2, [np.float32((-1.0) ** i / fact[2 * i + 1]) for i in range(8)])
    c = series(x2, [np.float32((-1.0) ** i / fact[2 * i]) for i in range(9)])
    return 1.0 - 2.0 * s * s, 2.0 * s * c


def step_kernel(dims, len_ref, lane_ref, x_ref, attn_g, kv_g, q_g, ffn_g, cache0, cache1, w_dkv, w_qa, w_qb, w_uk, w_uv, w_o, w_gate, w_up, w_down,
                x_out, entry_out, c_out0, c_out1,
                dkv_b, qa_b, qb_b, uk_b, uv_b, o_b, gate_b, up_b, down_b, s_b, mine_b, part_b, mid_b, all_b, send_b, sum_b,
                a_sems, f_sems, ps, pr, ms, mr, rs, rr):
    layers, rows, heads, nope, rope, lat, slots, tiles_all, tiles, ranks, tp, period = dims
    half = rope // 2
    hw = nope + rope
    width = heads * hw
    entry_w = lat + rope
    members = ranks * tp
    caches = (cache0, cache1)
    cache_b = (c_out0, c_out1)

    c = lax.axis_index("tp")
    d = lax.axis_index("dp")
    xx = lax.rem(d, SIDE)
    yy = lax.rem(d // SIDE, SIDE)
    pos = lax.rem(yy, 2) * 2 + lax.rem(xx, 2)
    corner = d - lax.rem(yy, 2) * SIDE - lax.rem(xx, 2)
    me = pos * tp + c

    def dp_of(q):
        return corner + (q // 2) * SIDE + lax.rem(q, 2)

    start = tiles_all * me // members
    count = tiles_all * (me + 1) // members - start
    base_tile = jnp.minimum(start, tiles_all - tiles)
    skip = start - base_tile
    first = pl.multiple_of(base_tile * LANES, LANES)

    qa_rows = w_qa.shape[1] // 2
    o_cuts = cuts(w_o.shape[1], 2)
    out_cuts = cuts(w_down.shape[2], 2)

    def attn_loads(layer):
        pairs = [("dkv", w_dkv.at[layer], dkv_b)]
        for i in range(2):
            cut = pl.ds(i * qa_rows, qa_rows)
            pairs.append((f"qa{i}", w_qa.at[layer, cut], qa_b.at[cut]))
        pairs.append(("qb", w_qb.at[layer], qb_b))
        pairs.append(("uk", w_uk.at[layer], uk_b.at[:, pl.ds(0, nope), pl.ds(0, lat)]))
        for r in range(rows):
            pairs.append((f"c{r}", caches[layer].at[r], cache_b[layer].at[r]))
        pairs.append(("uv", w_uv.at[layer], uv_b))
        for i, (at, size) in enumerate(o_cuts):
            cut = pl.ds(at, size)
            pairs.append((f"o{i}", w_o.at[layer, cut], o_b.at[cut]))
        loads = {name: pltpu.make_async_copy(a, b, a_sems.at[i]) for i, (name, a, b) in enumerate(pairs)}
        for load in loads.values():
            load.start()
        return loads

    def ffn_loads(layer):
        loads = [
            pltpu.make_async_copy(w_gate.at[layer, :, pl.ds(first, tiles * LANES)], gate_b, f_sems.at[0]),
            pltpu.make_async_copy(w_up.at[layer, :, pl.ds(first, tiles * LANES)], up_b, f_sems.at[1]),
            pltpu.make_async_copy(w_down.at[layer, pl.ds(first, tiles * LANES)], down_b, f_sems.at[2]),
        ]
        for load in loads:
            load.start()
        return loads

    a_loads = attn_loads(0)
    f_loads = ffn_loads(0)

    def peer(k):
        other = lax.rem(me + k, members)
        return other // tp, lax.rem(other, tp)

    barrier = pltpu.get_barrier_semaphore()
    for k in range(1, members):
        q, t = peer(k)
        pl.semaphore_signal(barrier, inc=1, device_id={"tp": t, "dp": dp_of(q)}, device_id_type=MESH)

    uk_b[:, nope:, :lat] = jnp.zeros((heads, rope, lat), BF16)
    sub = lax.broadcasted_iota(jnp.int32, (heads, hw, LANES), 1)
    lan = lax.broadcasted_iota(jnp.int32, (heads, hw, LANES), 2)
    uk_b[:, :, lat:] = jnp.where(sub == lan + nope, 1.0, 0.0).astype(BF16)
    entry_out[...] = jnp.zeros(entry_out.shape, F32)

    shape = (rows, period + LANES)
    row_id = lax.broadcasted_iota(jnp.int32, shape, 0)
    where_at = jnp.full(shape, len_ref[0].astype(F32))
    for r in range(1, rows):
        where_at = jnp.where(row_id == r, len_ref[r].astype(F32), where_at)
    turns = where_at * lane_ref[0:1, :]
    turns = (turns - jnp.floor(turns + 0.5)) + where_at * lane_ref[1:2, :]
    turns = turns - jnp.floor(turns + 0.5)
    cos_t, sin_t = cos_sin(turns)
    sin_t = sin_t * lane_ref[2:3, :]
    repeat = width // period
    cos_q = jnp.concatenate([cos_t[:, :period]] * repeat, axis=1)
    sin_q = jnp.concatenate([sin_t[:, :period]] * repeat, axis=1)
    cos_k, sin_k = cos_t[:, period:], sin_t[:, period:]
    sign_q = jnp.concatenate([jnp.broadcast_to(lane_ref[2:3, :period], (rows, period))] * repeat, axis=1)
    sign_k = jnp.broadcast_to(lane_ref[2:3, period:], (rows, LANES))

    spread_shape = (HEAD_PAD, width)
    head = lax.broadcasted_iota(jnp.int32, spread_shape, 0) * hw
    lane = lax.broadcasted_iota(jnp.int32, spread_shape, 1)
    spread_own = (lane >= head) & (lane < head + hw)
    v_dim = w_uv.shape[2]
    pick_shape = (HEAD_PAD, heads * v_dim)
    head = lax.broadcasted_iota(jnp.int32, pick_shape, 0) * v_dim
    lane = lax.broadcasted_iota(jnp.int32, pick_shape, 1)
    pick_own = (lane >= head) & (lane < head + v_dim)
    scale = hw ** -0.5
    x = x_ref[...].astype(F32)
    sends = []

    for layer in range(layers):
        cache = cache_b[layer]
        h = rms(x, attn_g[layer:layer + 1, :])
        a_loads["dkv"].wait()
        kv = dot_nt(h, dkv_b[...])
        k_lat = rms(kv[:, :lat], kv_g[layer:layer + 1, :])
        k_raw = jnp.concatenate([kv[:, lat:], jnp.zeros((rows, LANES - rope), F32)], axis=1)
        k_other = jnp.where(sign_k < 0, pltpu.roll(k_raw, LANES - half, 1), pltpu.roll(k_raw, half, 1))
        k_rot = (k_raw * cos_k + k_other * sin_k).astype(BF16)
        entry = jnp.concatenate([k_lat.astype(F32), k_rot.astype(F32)], axis=1)
        entry_out[layer * rows:(layer + 1) * rows, :] = entry

        qa = jnp.zeros((rows, w_qa.shape[2]), F32)
        for i in range(2):
            a_loads[f"qa{i}"].wait()
            qa += dot(h[:, i * qa_rows:(i + 1) * qa_rows], qa_b[pl.ds(i * qa_rows, qa_rows)])
        q_low = rms(qa, q_g[layer:layer + 1, :])
        a_loads["qb"].wait()
        q = dot(q_low, qb_b[...])
        q_other = jnp.where(sign_q < 0, pltpu.roll(q, width - half, 1), pltpu.roll(q, half, 1))
        q = q * cos_q + q_other * sin_q
        spread = jnp.concatenate([jnp.where(spread_own, jnp.broadcast_to(q[r:r + 1], spread_shape), 0.0) for r in range(rows)], axis=0).astype(BF16)
        a_loads["uk"].wait()
        query = dot(spread, uk_b[...].reshape(width, lat + LANES))

        tail = query[:, lat:]
        group = lax.broadcasted_iota(jnp.int32, tail.shape, 0)
        rotary = tail
        for r in range(1, rows):
            rotary = jnp.where(group >= r * HEAD_PAD, pltpu.roll(tail, r * rope, 1), rotary)
        rotary = rotary[:, :rows * rope].astype(BF16)
        q_rows = [query[r * HEAD_PAD:(r + 1) * HEAD_PAD].astype(BF16) for r in range(rows)]
        s_new = [jnp.sum(q_rows[r].astype(F32) * entry[r:r + 1], axis=1, keepdims=True) * scale for r in range(rows)]
        top = list(s_new)
        for r in range(rows):
            a_loads[f"c{r}"].wait()
        for k in range(slots // CHUNK):
            cols = pl.ds(k * CHUNK, CHUNK)
            stacked = jnp.concatenate([cache[r, pl.ds(lat, rope), cols] for r in range(rows)], axis=0)
            s_rot = dot(rotary, stacked)
            for r in range(rows):
                s = dot(q_rows[r][:, :lat], cache[r, pl.ds(0, lat), cols]) + s_rot[r * HEAD_PAD:(r + 1) * HEAD_PAD]
                slot = lax.broadcasted_iota(jnp.int32, s.shape, 1) + k * CHUNK
                s = jnp.where(slot < len_ref[r], s * scale, -1e30)
                s_b[r, :, cols] = s
                top[r] = jnp.maximum(top[r], jnp.max(s, axis=1, keepdims=True))
        o_lat = []
        for r in range(rows):
            e_new = jnp.exp(s_new[r] - top[r])
            total = e_new
            for k in range(slots // CHUNK):
                cols = pl.ds(k * CHUNK, CHUNK)
                e = jnp.exp(s_b[r, :, cols] - top[r])
                s_b[r, :, cols] = e
                total += jnp.sum(e, axis=1, keepdims=True)
            inv = 1.0 / total
            acc = (e_new * inv).astype(BF16).astype(F32) * entry[r:r + 1, :lat]
            for k in range(slots // CHUNK):
                cols = pl.ds(k * CHUNK, CHUNK)
                p = (s_b[r, :, cols] * inv).astype(BF16)
                acc += dot_nt(p, cache[r, pl.ds(0, lat), cols])
            o_lat.append(acc)
        o_lat = jnp.concatenate(o_lat, axis=0).astype(BF16)
        a_loads["uv"].wait()
        wide = dot_nt(o_lat, uv_b[...].reshape(heads * v_dim, lat))
        o = [jnp.sum(jnp.where(pick_own, wide[r * HEAD_PAD:(r + 1) * HEAD_PAD], 0.0), axis=0, keepdims=True) for r in range(rows)]
        o = jnp.concatenate(o, axis=0).astype(BF16)
        part = x * jnp.where(c == 0, 1.0, 0.0)
        for i, (at, size) in enumerate(o_cuts):
            a_loads[f"o{i}"].wait()
            part += dot(o[:, at:at + size], o_b[pl.ds(at, size)])

        mine_b[layer] = part
        if layer == 0:
            pl.semaphore_wait(barrier, members - 1)
        swap = pltpu.make_async_remote_copy(
            src_ref=mine_b.at[layer], dst_ref=part_b.at[layer], send_sem=ps.at[layer], recv_sem=pr.at[layer],
            device_id={"tp": 1 - c, "dp": d}, device_id_type=MESH)
        swap.start()
        if layer + 1 < layers:
            a_loads = attn_loads(layer + 1)
        swap.wait_recv()
        x_mid = (part + part_b[layer]).astype(BF16)
        mid_b[layer, pos] = x_mid

        gathers = []
        for k in range(1, ranks):
            q = lax.rem(pos + k, ranks)
            for t in range(tp):
                gathers.append(pltpu.make_async_remote_copy(
                    src_ref=mid_b.at[layer, pos], dst_ref=mid_b.at[layer, pos], send_sem=ms.at[layer, k - 1, t], recv_sem=mr.at[layer, k - 1],
                    device_id={"tp": t, "dp": dp_of(q)}, device_id_type=MESH))

        @pl.when(c == tp - 1)
        def _():
            for copy in gathers:
                copy.start()
        for k in range(ranks - 1):
            gathers[k * tp].wait_recv()

        for q in range(ranks):
            all_b[q * rows:(q + 1) * rows, :] = mid_b[layer, q].astype(F32)
        g = rms(all_b[...], ffn_g[layer:layer + 1, :])
        f_loads[0].wait()
        whole = tiles * LANES // PASS * PASS
        a = dot(g, gate_b[:, :whole])
        f_loads[1].wait()
        b = dot(g, up_b[:, :whole])
        if whole < tiles * LANES:
            both = dot(g, jnp.concatenate([gate_b[:, whole:], up_b[:, whole:]], axis=1))
            a = jnp.concatenate([a, both[:, :LANES]], axis=1)
            b = jnp.concatenate([b, both[:, LANES:]], axis=1)
        lane = lax.broadcasted_iota(jnp.int32, a.shape, 1)
        kept = (lane >= skip * LANES) & (lane < (skip + count) * LANES)
        u = jnp.where(kept, a * jax.nn.sigmoid(a) * b, 0.0).astype(BF16)
        f_loads[2].wait()
        returns = []
        for n, (at, size) in enumerate(out_cuts):
            cut = pl.ds(at, size)
            partial = dot(u, down_b[:, at:at + size])
            for q in range(ranks):
                send_b[layer, q, :, at:at + size] = partial[q * rows:(q + 1) * rows].astype(BF16)
            sum_b[layer, me, :, at:at + size] = send_b[layer, pos, :, at:at + size]
            piece = []
            for k in range(1, members):
                q, t = peer(k)
                piece.append(pltpu.make_async_remote_copy(
                    src_ref=send_b.at[layer, q, :, cut], dst_ref=sum_b.at[layer, me, :, cut],
                    send_sem=rs.at[layer, n, k - 1], recv_sem=rr.at[layer, n, k - 1],
                    device_id={"tp": t, "dp": dp_of(q)}, device_id_type=MESH))
            for copy in piece:
                copy.start()
            returns.append(piece)
        if layer + 1 < layers:
            f_loads = ffn_loads(layer + 1)
        totals = []
        for (at, size), piece in zip(out_cuts, returns):
            for copy in piece:
                copy.wait_recv()
            total = sum_b[layer, 0, :, at:at + size].astype(F32)
            for j in range(1, members):
                total = total + sum_b[layer, j, :, at:at + size].astype(F32)
            totals.append(total)
        total = jnp.concatenate(totals, axis=1)
        x_new = (x_mid.astype(F32) + total).astype(BF16)
        x = x_new.astype(F32)
        sends.append((swap, gathers, sum(returns, [])))

    x_out[...] = x_new
    for swap, gathers, returns in sends:
        swap.wait_send()
        for copy in returns:
            copy.wait_send()

        @pl.when(c == tp - 1)
        def _():
            for copy in gathers:
                copy.wait_send()


def write_kernel(dims, len_ref, x_ref, entry_ref, c0, c1, x_out, out0, out1, patch_b, x_sem, sems):
    layers, rows, entry_w, slots = dims
    x_copy = pltpu.make_async_copy(x_ref, x_out, x_sem.at[0])
    x_copy.start()
    entry_t = entry_ref[...].T[:entry_w]
    caches, outs = (c0, c1), (out0, out1)
    for layer in range(layers):
        for r in range(rows):
            length = len_ref[r]
            home = length // OUT_CHUNK
            for k in range(slots // OUT_CHUNK):
                cols = pl.ds(k * OUT_CHUNK, OUT_CHUNK)

                @pl.when(home != k)
                def _():
                    pltpu.make_async_copy(caches[layer].at[r, :, cols], outs[layer].at[r, :, cols], sems.at[layer, r]).start()
    for layer in range(layers):
        for r in range(rows):
            length = len_ref[r]
            base = pl.multiple_of(length // OUT_CHUNK * OUT_CHUNK, OUT_CHUNK)
            tile = caches[layer][r, :, pl.ds(base, OUT_CHUNK)].astype(F32)
            lane = lax.broadcasted_iota(jnp.int32, tile.shape, 1)
            column = entry_t[:, layer * rows + r:layer * rows + r + 1]
            patch_b[layer, r] = jnp.where(lane == length - base, jnp.broadcast_to(column, tile.shape), tile).astype(BF16)
            pltpu.make_async_copy(patch_b.at[layer, r], outs[layer].at[r, :, pl.ds(base, OUT_CHUNK)], sems.at[layer, r]).start()
    for layer in range(layers):
        for r in range(rows):
            pltpu.make_async_copy(caches[layer].at[r], outs[layer].at[r], sems.at[layer, r]).wait()
    x_copy.wait()


def solution(mesh):
    tp_size = mesh.shape['tp']
    ranks = 4
    row_spec = P(('rep', 'dp'), None)
    cache_spec = P(('rep', 'dp'), None, None)
    in_specs = (row_spec, P(('rep', 'dp')), cache_spec, cache_spec, P(), P(), P(), P(), P(), P(), P(None, None, 'tp'), P(None, 'tp', None, None), P(None, 'tp', None, None), P(None, 'tp', None), P(), P(), P())
    out_specs = (row_spec, cache_spec, cache_spec)

    def local_step(x, lengths, cache0, cache1, attn_gain, kv_gain, q_gain, ffn_gain, w_dkv, w_qa, w_qb, w_uk, w_uv, w_o, w_gate, w_up, w_down):
        rows, model = x.shape
        layers, heads, nope, lat = w_uk.shape
        slots = cache0.shape[1]
        rope = cache0.shape[2] - lat
        hw = nope + rope
        period = int(np.lcm(hw, LANES))
        tiles_all = w_gate.shape[2] // LANES
        members = ranks * tp_size
        tiles = -(-tiles_all // members)
        lanes = jnp.asarray(rope_lanes(hw, nope, rope, period))
        c0, c1 = jnp.swapaxes(cache0, 1, 2), jnp.swapaxes(cache1, 1, 2)
        w_dkv_t = jnp.swapaxes(w_dkv, 1, 2)
        w_uv_t = jnp.swapaxes(w_uv, 2, 3)
        dims = (layers, rows, heads, nope, rope, lat, slots, tiles_all, tiles, ranks, tp_size, period)
        dma = pltpu.SemaphoreType.DMA
        x_new, entries, held0, held1 = pl.pallas_call(
            functools.partial(step_kernel, dims),
            name="step",
            out_shape=(pltpu.VMEM((rows, model), BF16), pltpu.VMEM((8, lat + LANES), F32), pltpu.VMEM(c0.shape, BF16), pltpu.VMEM(c1.shape, BF16)),
            in_specs=[SMEM_SPEC] + [VMEM_SPEC] * 6 + [HBM_SPEC] * 11,
            out_specs=(VMEM_SPEC, VMEM_SPEC, VMEM_SPEC, VMEM_SPEC),
            scratch_shapes=[
                pltpu.VMEM(w_dkv_t.shape[1:], BF16),
                pltpu.VMEM(w_qa.shape[1:], BF16),
                pltpu.VMEM(w_qb.shape[1:], BF16),
                pltpu.VMEM((heads, hw, lat + LANES), BF16),
                pltpu.VMEM(w_uv_t.shape[1:], BF16),
                pltpu.VMEM(w_o.shape[1:], BF16),
                pltpu.VMEM((model, tiles * LANES), BF16),
                pltpu.VMEM((model, tiles * LANES), BF16),
                pltpu.VMEM((tiles * LANES, model), BF16),
                pltpu.VMEM((rows, HEAD_PAD, slots), F32),
                pltpu.VMEM((layers, rows, model), F32),
                pltpu.VMEM((layers, rows, model), F32),
                pltpu.VMEM((layers, ranks, rows, model), BF16),
                pltpu.VMEM((ranks * rows, model), F32),
                pltpu.VMEM((layers, ranks, rows, model), BF16),
                pltpu.VMEM((layers, members, rows, model), BF16),
                dma((10,)),
                dma((3,)),
                dma((layers,)),
                dma((layers,)),
                dma((layers, ranks - 1, tp_size)),
                dma((layers, ranks - 1)),
                dma((layers, 2, members - 1)),
                dma((layers, 2, members - 1)),
            ],
            compiler_params=pltpu.CompilerParams(collective_id=0, has_side_effects=True, vmem_limit_bytes=46 * 2 ** 20),
            cost_estimate=pl.CostEstimate(flops=10 ** 9, bytes_accessed=70 * 10 ** 6, transcendentals=4 * 10 ** 5),
        )(lengths, lanes, x, attn_gain, kv_gain, q_gain, ffn_gain, c0, c1, w_dkv_t, w_qa, w_qb, w_uk, w_uv_t, w_o, w_gate, w_up, w_down)
        x_new, new0, new1 = pl.pallas_call(
            functools.partial(write_kernel, (layers, rows, lat + rope, slots)),
            name="write",
            out_shape=(jax.ShapeDtypeStruct(x.shape, BF16), jax.ShapeDtypeStruct(c0.shape, BF16), jax.ShapeDtypeStruct(c1.shape, BF16)),
            in_specs=[SMEM_SPEC, VMEM_SPEC, VMEM_SPEC, VMEM_SPEC, VMEM_SPEC],
            out_specs=(HBM_SPEC, HBM_SPEC, HBM_SPEC),
            scratch_shapes=[pltpu.VMEM((layers, rows, lat + rope, OUT_CHUNK), BF16), dma((1,)), dma((layers, rows))],
            compiler_params=pltpu.CompilerParams(vmem_limit_bytes=24 * 2 ** 20),
            cost_estimate=pl.CostEstimate(flops=10 ** 6, bytes_accessed=20 * 10 ** 6, transcendentals=0),
        )(lengths, x_new, entries, held0, held1)
        return x_new, jnp.swapaxes(new0, 1, 2), jnp.swapaxes(new1, 1, 2)

    return jax.shard_map(local_step, mesh=mesh, in_specs=in_specs, out_specs=out_specs, check_vma=False)
```
